32 devices in a mesh: row: 4 (over z), col: 2 (over y), layer: 4 (over x, core).
Axes of the slice: x: 2, y: 2, z: 4, core: 2. Of those that a mesh axis runs over, the one named last changes fastest.
Arguments:
- amplitudes: float32 [2016, 73536], P('row', ('layer', 'col')), may hold values from -6 to 6
- integrals: float32 [73536, 768], P(('layer', 'col'), 'row'), may hold values from -0.03125 to 0.03125
- occ_energy: float32 [64], replicated, may hold values from -2 to -0.5
- vir_energy: float32 [384], replicated, may hold values from 0.2 to 3
Outputs:
- ladder: float32 [2016, 768], P('col', ('row', 'layer'))
- amplitude_step: float32 [2016, 768], P('col', ('row', 'layer'))
The draws below stay inside these ranges and needn't reach their ends.
All inputs are finite; a program needn't handle non-finite values.
Results may differ from the reference program's by a relative error of at most 0.00007.
Values sent between devices are 32-bit elements; how exact they have to be, the bound alone decides.
No kernel may reach another device: no remote copies, remote signals or barrier semaphores. Data moves between devices by JAX's collectives and lax.ppermute only.
A program may use at most 128 MiB of HBM per device.

```python
import jax
import jax.numpy as jnp
import numpy as np
from jax import lax

NO = 64
NV = 384
IJ = 2016
K = 73536
AB = 768


def spiked(values, stream_key, source, target, parts, factor):
    def block_of(dim):
        return (jnp.arange(values.shape[dim]) // (values.shape[dim] // parts)).reshape((-1,) + (1,) * (values.ndim - 1 - dim))

    one_side = jax.random.permutation(stream_key, parts)[block_of(target)]
    far = (block_of(target) + parts // 2) % parts
    return jnp.where((block_of(source) == one_side) | (block_of(source) == far), factor * values, values)


def level_of(stream_key, shape, pieces, low, top_value):
    level, own = 1.0, jax.random.fold_in(stream_key, 6)
    for axis_at, parts in pieces:
        steps = jnp.exp(jax.random.uniform(jax.random.fold_in(own, axis_at), (parts,), jnp.float32, low / len(pieces), top_value / len(pieces)))
        level = level * jnp.repeat(steps, shape[axis_at] // parts).reshape([-1 if axis == axis_at else 1 for axis in range(len(shape))])
    return level


def gaussian(own_key, shape, deviation, limit, shards=(), kind=jnp.bfloat16):
    result = jax.random.normal(own_key, shape, jnp.float32) * deviation
    if len(shards) > 0:
        result = level_of(own_key, shape, shards, -0.22, 0.18) * result
    return jnp.clip(result, min=-limit, max=limit).astype(kind)


def noise_with(key, shape, deviation, reach, split, heavy, kind=jnp.bfloat16):
    values = deviation * jax.random.normal(key, shape, jnp.float32)
    if split:
        values = values * level_of(key, shape, split, -0.22, 0.18)
    return jnp.clip(spiked(values, jax.random.fold_in(key, 3), *heavy), -reach, reach).astype(kind)


def setup_inputs(seed: int = 0) -> dict:
    seeds = jax.random.split(jax.random.key(seed), 5)
    return {
        "amplitudes": gaussian(seeds[0], (IJ, K), 1.0, 6.0, ((0, 4), (1, 8)), jnp.float32),
        "integrals": noise_with(seeds[1], (K, AB), K ** -0.5, 0.03125, ((0, 8), (1, 4)), (0, 1, 8, 2.0), jnp.float32),
        "occ_energy": jnp.clip(jax.random.uniform(seeds[2], (NO,), jnp.float32, -2.0, -0.5), -2.0, -0.5),
        "vir_energy": jnp.clip(jax.random.uniform(seeds[3], (NV,), jnp.float32, 0.2, 3.0), 0.2, 3.0),
    }


def reference(amplitudes, integrals, occ_energy, vir_energy):
    first_np, second_np = np.triu_indices(NO, 1)
    first_index = jnp.asarray(first_np, dtype=jnp.int32)
    second_index = jnp.asarray(second_np, dtype=jnp.int32)
    ladder = jnp.dot(amplitudes, integrals, precision=lax.Precision.HIGHEST, preferred_element_type=jnp.float32)
    pair_sum = occ_energy[first_index] + occ_energy[second_index]
    ab_index = jnp.arange(AB, dtype=jnp.int32)
    vir_sum = vir_energy[ab_index // NV] + vir_energy[ab_index % NV]
    denominator = pair_sum[:, None] - vir_sum[None, :]
    return ladder, ladder / denominator
```

```python
import jax
import jax.numpy as jnp
import numpy as np
from jax import lax
from jax.sharding import PartitionSpec as P


def lookup(indices, values_table):
    positions = jnp.arange(values_table.shape[0], dtype=jnp.int32)
    picked = jnp.where(indices[:, None] == positions[None, :], values_table[None, :], 0.0)
    return jnp.sum(picked, axis=1)


def product(integral_chunk, amplitude_chunk):
    return lax.dot_general(
        integral_chunk,
        amplitude_chunk,
        (((0,), (1,)), ((), ())),
        precision=lax.Precision.HIGH,
        preferred_element_type=jnp.float32,
    )


def total(parts):
    return sum(parts[1:], parts[0])


def chunk_bounds(depth):
    kept = depth * 21 // 32
    first = depth // 18
    if depth >= 4096:
        kept -= kept % 128
        first -= first % 128
    half = kept // 2
    if depth >= 4096:
        half -= half % 128
    return [0, first, half, kept, depth]


def streamed_blocks(amplitudes, integrals):
    rows = lax.axis_size("row")
    plane = lax.axis_index("row")
    bounds = chunk_bounds(integrals.shape[0])
    spans = list(zip(bounds[:-1], bounds[1:]))
    last = len(spans) - 1
    own = [integrals[a:b] for a, b in spans]
    amps = [amplitudes[:, a:b] for a, b in spans]

    def hop(values, distance, c):
        low, high = (1, rows - 2) if c == last else (0, rows - 1)
        up = [(p - 1, p) for p in range(distance, rows) if low <= p <= high]
        down = [(rows - 1 - p, rows - 1 - t) for p, t in up]
        return lax.ppermute(values[0], "row", up), lax.ppermute(values[1], "row", down)

    near = [hop((own[c], own[c]), 1, c) for c in range(last + 1)]
    lent = lax.ppermute(amps[last], "row", [(0, 1), (rows - 1, rows - 2)])
    middle = [total(hop(near[c], 2, c)) for c in range(last + 1)]
    far = [lax.ppermute(middle[c], "row", [(1, 0), (rows - 2, rows - 1)]) for c in range(last)]

    lower = plane < rows // 2
    at_end = (plane == 0) | (plane == rows - 1)
    self_block = total([product(own[c], amps[c]) for c in range(last + 1)])
    from_below = total([product(near[c][0], amps[c]) for c in range(last + 1)])
    from_above = total([product(near[c][1], amps[c]) for c in range(last + 1)])
    middle_block = total([product(middle[c], amps[c]) for c in range(last)])
    far_block = total([product(far[c], amps[c]) for c in range(last)])
    second = jnp.where(at_end, middle_block, 0.0)
    late = jnp.where(at_end, far_block, middle_block) + product(middle[last], amps[last])
    lent_self = product(own[last], lent)
    lent_near = product(jnp.where(lower, near[last][1], near[last][0]), lent)
    lent_late = product(middle[last], lent)
    return (self_block, from_above, from_below), (second, lent_self, lent_near), (late, lent_late)


def plane_sums(blocks):
    layers, cols = lax.axis_size("layer"), lax.axis_size("col")
    layer, col = lax.axis_index("layer"), lax.axis_index("col")
    share = blocks[0].shape[0] // (layers * cols)
    pairs = layers // 2
    stacked = jnp.stack(blocks).reshape(len(blocks), pairs, 2, cols, share, -1)

    def pick(values, place, axis):
        return lax.dynamic_index_in_dim(values, place, axis, keepdims=False)

    core = layer % 2
    halves = pick(stacked, core, 2) + lax.ppermute(
        pick(stacked, 1 - core, 2), "layer", [(n, n ^ 1) for n in range(layers)]
    )
    pair = layer // 2

    def piece(pair_at, col_at):
        return pick(pick(halves, pair_at, 1), col_at, 1)

    sums = piece(pair, col)
    for pair_step in range(pairs):
        for col_step in range(cols):
            if pair_step or col_step:
                moves = [
                    (
                        c * layers + n,
                        (c + col_step) % cols * layers + ((n // 2 + pair_step) % pairs) * 2 + n % 2,
                    )
                    for c in range(cols)
                    for n in range(layers)
                ]
                sent = piece((pair + pair_step) % pairs, (col + col_step) % cols)
                sums = sums + lax.ppermute(sent, ("col", "layer"), moves)
    return [sums[k] for k in range(len(blocks))]


def owned_columns(early, middle, late):
    rows = lax.axis_size("row")
    end = rows - 1
    plane = lax.axis_index("row")
    self_block, to_above, to_below = plane_sums(early)
    second, lent_self, lent_near = plane_sums(middle)
    last, lent_last = plane_sums(late)
    from_below = lax.ppermute(to_above, "row", [(p, p + 1) for p in range(end)])
    from_above = lax.ppermute(to_below, "row", [(p + 1, p) for p in range(end)])
    second = lax.ppermute(second, "row", [(0, 2), (end, end - 2)])
    lent_near = lax.ppermute(lent_near, "row", [(1, 2), (2, 1)])
    from_far = lax.ppermute(last, "row", [(0, end), (end, 0)])
    from_second = lax.ppermute(jnp.stack([last, lent_last]), "row", [(1, end), (2, 0)])
    from_end = from_far + from_second[1] + second + lent_near
    tables = (
        (self_block, from_above, from_second[0], from_end),
        (from_below + lent_self, self_block, from_above, from_end),
        (from_end, from_below, self_block, from_above + lent_self),
        (from_end, from_second[0], from_below, self_block),
    )
    chosen = []
    for source in range(rows):
        value = tables[0][source]
        for p in range(1, rows):
            value = jnp.where(plane == p, tables[p][source], value)
        chosen.append(value)
    return jnp.stack(chosen)


def ladder_by_plane_sums(amplitudes, integrals):
    cols, col = lax.axis_size("col"), lax.axis_index("col")
    owned = owned_columns(*streamed_blocks(amplitudes, integrals))
    rows, share, height = owned.shape
    group = rows // cols
    by_col = owned.reshape(cols, group, share, height)
    halves = []
    for step in range(cols):
        sent = lax.dynamic_index_in_dim(by_col, (col + step) % cols, 0, keepdims=False)
        if step:
            sent = lax.ppermute(sent, "col", [(c, (c + step) % cols) for c in range(cols)])
        halves.append(sent)
    ordered = jnp.stack(halves[::-1])
    ordered = jnp.roll(ordered, col + 1, axis=0)
    return ordered.transpose(1, 3, 0, 2).reshape(group * height, cols * share)


def ladder_by_scatter(amplitudes, integrals):
    partial_rows = jnp.dot(
        amplitudes,
        lax.all_gather(integrals, "row", axis=1, tiled=True),
        precision=lax.Precision.HIGHEST,
        preferred_element_type=jnp.float32,
    )
    partial_sum = lax.all_to_all(partial_rows, "row", split_axis=1, concat_axis=0, tiled=True)
    col_count = lax.axis_size("col")
    layer_count = lax.axis_size("layer")
    pair_rows = partial_sum.shape[0] // col_count
    slab_cols = partial_sum.shape[1] // layer_count
    blocks = partial_sum.reshape(col_count, pair_rows, layer_count, slab_cols)
    blocks = blocks.transpose(0, 2, 1, 3).reshape(col_count * layer_count * pair_rows, slab_cols)
    return lax.psum_scatter(blocks, ("col", "layer"), scatter_dimension=0, tiled=True)


def denominators(occ_energy, vir_energy, pair_rows, slab_cols):
    occupied = occ_energy.shape[0]
    virtuals = vir_energy.shape[0]
    first_np, second_np = np.triu_indices(occupied, 1)
    ij_start = lax.axis_index("col") * pair_rows
    ab_start = (
        lax.axis_index("row") * lax.axis_size("layer") + lax.axis_index("layer")
    ) * slab_cols
    first_index = lax.dynamic_slice_in_dim(
        jnp.asarray(first_np, dtype=jnp.int32), ij_start, pair_rows
    )
    second_index = lax.dynamic_slice_in_dim(
        jnp.asarray(second_np, dtype=jnp.int32), ij_start, pair_rows
    )
    pair_sum = lookup(first_index, occ_energy) + lookup(second_index, occ_energy)
    ab_index = ab_start + jnp.arange(slab_cols, dtype=jnp.int32)
    vir_sum = lookup(ab_index // virtuals, vir_energy) + lookup(ab_index % virtuals, vir_energy)
    return pair_sum[:, None] - vir_sum[None, :]


def shards(amplitudes, integrals, occ_energy, vir_energy):
    rows, cols, layers = (lax.axis_size(name) for name in ("row", "col", "layer"))
    in_planes = rows == 4 and rows % cols == 0 and layers % 2 == 0
    if in_planes and integrals.shape[1] % (cols * layers) == 0:
        ladder = ladder_by_plane_sums(amplitudes, integrals)
    else:
        ladder = ladder_by_scatter(amplitudes, integrals)
    denominator = denominators(occ_energy, vir_energy, ladder.shape[0], ladder.shape[1])
    return (ladder, ladder / denominator)


def solution(mesh):
    in_specs = (P("row", ("layer", "col")), P(("layer", "col"), "row"), P(), P())
    out_specs = (P("col", ("row", "layer")), P("col", ("row", "layer")))
    return jax.shard_map(shards, mesh=mesh, in_specs=in_specs, out_specs=out_specs, check_vma=False)
```

```python
import functools

import jax
import jax.numpy as jnp
import numpy as np
from jax import lax
from jax.experimental import pallas as pl
from jax.experimental.pallas import tpu as pltpu
from jax.sharding import PartitionSpec as P


ROW, COL, LAYER = "row", "col", "layer"


def lookup(indices, values_table):
    positions = jnp.arange(values_table.shape[0], dtype=jnp.int32)
    picked = jnp.where(indices[:, None] == positions[None, :], values_table[None, :], 0.0)
    return jnp.sum(picked, axis=1)


def split(values):
    high = values.astype(jnp.bfloat16)
    return high, (values - high.astype(jnp.float32)).astype(jnp.bfloat16)


def product_kernel(depth, step, term_sizes, flag_ref, *refs):
    at = pl.program_id(0)
    term_refs = refs[: sum(term_sizes)]
    source_ref = refs[len(term_refs)]
    start_refs = refs[len(term_refs) + 1 : -1]
    total_ref = refs[-1]

    def valid(values):
        if depth % step == 0:
            return values
        place = lax.broadcasted_iota(jnp.int32, values.shape, 1)
        return jnp.where(place < depth - at * step, values, 0.0)

    blocks = []
    used = 0
    for size in term_sizes:
        block = term_refs[used][...]
        if size == 2:
            other = term_refs[used + 1][...]
            block = jnp.where(flag_ref[0] == 2, block + other, jnp.where(flag_ref[0] == 1, other, block))
        blocks.append(split(valid(block)))
        used += size
    high, low = split(valid(source_ref[...]))

    def dot(a, b):
        return lax.dot_general(a, b, (((1,), (1,)), ((), ())), preferred_element_type=jnp.float32)

    left_high = jnp.concatenate([block for block, _ in blocks], axis=0)
    left = jnp.concatenate([left_high] + [block for _, block in blocks], axis=0)
    half = left_high.shape[0]
    both = dot(left, high)
    part = both[:half] + (both[half:] + dot(left_high, low))

    @pl.when(at == 0)
    def _():
        total_ref[...] = part if not start_refs else start_refs[0][...] + part

    @pl.when(at > 0)
    def _():
        total_ref[...] += part


def products(terms, source, offset, start=None, flag=None):
    chunks = [chunk for term in terms for chunk in term]
    depth, columns = chunks[0].shape
    height = source.shape[0]
    step = next(n for n in (512, 256, 128) if offset % n == 0)
    if depth % step and depth % 256 == 0:
        step = 256
    in_specs = [pl.BlockSpec((columns, step), lambda i, _: (0, i))] * len(chunks)
    in_specs.append(pl.BlockSpec((height, step), lambda i, _: (0, offset // step + i)))
    shape = (len(terms) * columns, height)
    whole = pl.BlockSpec(shape, lambda i, _: (0, 0))
    operands = [chunk.T for chunk in chunks] + [source]
    aliases = {}
    if start is not None:
        aliases = {1 + len(operands): 0}
        in_specs.append(whole)
        operands.append(start)
    flags = jnp.full((1,), 2, jnp.int32) if flag is None else flag.reshape(1).astype(jnp.int32)
    return pl.pallas_call(
        functools.partial(product_kernel, depth, step, tuple(len(t) for t in terms)),
        grid_spec=pltpu.PrefetchScalarGridSpec(
            num_scalar_prefetch=1,
            grid=(pl.cdiv(depth, step),),
            in_specs=in_specs,
            out_specs=whole,
        ),
        out_shape=jax.ShapeDtypeStruct(shape, jnp.float32),
        input_output_aliases=aliases,
        compiler_params=pltpu.CompilerParams(dimension_semantics=("arbitrary",)),
        cost_estimate=pl.CostEstimate(
            flops=2 * depth * shape[0] * height,
            bytes_accessed=4 * depth * (columns * len(chunks) + height),
            transcendentals=0,
        ),
    )(flags, *operands)


def product(chunk, source):
    return lax.dot_general(
        chunk,
        source,
        (((0,), (1,)), ((), ())),
        precision=lax.Precision.HIGH,
        preferred_element_type=jnp.float32,
    )


def total(parts):
    return sum(parts[1:], parts[0])


CHUNKS = 4
KEPT = 2


def chunk_bounds(depth):
    tile = 256
    ends = [depth * share // 1024 // tile * tile for share in (314, 656, 913)]
    return [0] + ends + [depth]


def streamed_blocks(amplitudes, integrals):
    rows = lax.axis_size(ROW)
    plane = lax.axis_index(ROW)
    bounds = chunk_bounds(integrals.shape[0])
    own = [integrals[a:b] for a, b in zip(bounds[:-1], bounds[1:])]

    def hop(values, distance, c):
        low, high = (0, rows - 1) if c < KEPT else (1, rows - 2)
        up = [(p - 1, p) for p in range(distance, rows) if low <= p <= high]
        down = [(rows - 1 - p, rows - 1 - t) for p, t in up]
        upward = lax.ppermute(values[0], ROW, up)
        downward = lax.ppermute(values[1], ROW, down)
        return upward, downward

    near, lent = [], {}
    for c in range(CHUNKS):
        near.append(hop((own[c], own[c]), 1, c))
    for c in range(KEPT, CHUNKS):
        sent = amplitudes[:, bounds[c] : bounds[c + 1]]
        lent[c] = lax.ppermute(sent, ROW, [(0, 1), (rows - 1, rows - 2)])
    middle = [hop(near[c], 2, c) for c in range(CHUNKS)]
    far = [hop(middle[c], 3, c) for c in range(KEPT)]

    lower = (plane < rows // 2).astype(jnp.int32)
    at_end = (plane == 0) | (plane == rows - 1)
    slab = integrals.shape[1]
    self_block = products([(integrals,)], amplitudes, 0)
    nearby, second, lent_inner = None, None, None
    for c in range(CHUNKS):
        nearby = products([(near[c][0],), (near[c][1],)], amplitudes, bounds[c], nearby)
    for c in range(KEPT - 1):
        second = products([middle[c]], amplitudes, bounds[c], second)
    a, b = bounds[KEPT - 1 : KEPT + 1]
    second = second + product(total(middle[KEPT - 1]), amplitudes[:, a:b])
    second = lax.optimization_barrier(second)
    end = CHUNKS - 1
    for c in range(KEPT, end):
        lent_inner = products([(own[c],), near[c]], lent[c], 0, lent_inner, lower)
    late = jnp.where(at_end, 0.0, second)
    second = jnp.where(at_end, second, 0.0)
    for c in range(KEPT - 1):
        late = late + product(total(far[c]), amplitudes[:, bounds[c] : bounds[c + 1]])
    late = lax.optimization_barrier(late)
    lent_late = 0.0
    for c in range(KEPT, end):
        chunk = total(middle[c])
        late = late + product(chunk, amplitudes[:, bounds[c] : bounds[c + 1]])
        lent_late = lent_late + product(chunk, lent[c])
        late, lent_late = lax.optimization_barrier((late, lent_late))
    chosen = jnp.where(plane < rows // 2, near[end][1], near[end][0])
    lent_self = lent_inner[:slab] + product(own[end], lent[end])
    lent_near = lent_inner[slab:] + product(chosen, lent[end])
    late = late + product(total(far[KEPT - 1]), amplitudes[:, a:b])
    chunk = total(middle[end])
    late = late + product(chunk, amplitudes[:, bounds[end] :])
    lent_late = lent_late + product(chunk, lent[end])
    return (self_block, nearby[slab:], nearby[:slab]), (late, lent_late, second + lent_self, lent_near)


def plane_sums(blocks):
    layers, cols = lax.axis_size(LAYER), lax.axis_size(COL)
    layer, col = lax.axis_index(LAYER), lax.axis_index(COL)
    share = blocks[0].shape[0] // (layers * cols)
    pairs = layers // 2
    stacked = jnp.stack(blocks).reshape(len(blocks), pairs, 2, cols, share, -1)

    def pick(values, place, axis):
        return lax.dynamic_index_in_dim(values, place, axis, keepdims=False)

    core = layer % 2
    other = lax.ppermute(pick(stacked, 1 - core, 2), LAYER, [(n, n ^ 1) for n in range(layers)])
    halves = pick(stacked, core, 2) + other
    pair = layer // 2

    def piece(pair_at, col_at):
        return pick(pick(halves, pair_at, 1), col_at, 1)

    sums = piece(pair, col)
    for pair_step in range(pairs):
        for col_step in range(cols):
            if pair_step or col_step:
                moves = [
                    (
                        c * layers + n,
                        (c + col_step) % cols * layers + ((n // 2 + pair_step) % pairs) * 2 + n % 2,
                    )
                    for c in range(cols)
                    for n in range(layers)
                ]
                sent = piece((pair + pair_step) % pairs, (col + col_step) % cols)
                sums = sums + lax.ppermute(sent, (COL, LAYER), moves)
    return sums


def to_owner_col(values):
    rows, cols = lax.axis_size(ROW), lax.axis_size(COL)
    col, plane = lax.axis_index(COL), lax.axis_index(ROW)
    owners = [p * cols // rows for p in range(rows)]
    pairs = [(p * cols + (owners[p] + 1) % cols, p * cols + owners[p]) for p in range(rows)]
    other = lax.ppermute(values, (ROW, COL), pairs)
    first = col == 0
    both = jnp.stack([jnp.where(first, values, other), jnp.where(first, other, values)])
    return jnp.where(col == plane * cols // rows, both, 0.0)


def between_planes(values, moves):
    rows, cols = lax.axis_size(ROW), lax.axis_size(COL)
    pairs = [(s * cols + s * cols // rows, t * cols + s * cols // rows) for s, t in moves]
    return lax.ppermute(values, (ROW, COL), pairs)


def to_owner(values, moves):
    rows, cols = lax.axis_size(ROW), lax.axis_size(COL)
    arrived = []
    for step in range(cols):
        owners = [(s, t, s * cols // rows) for s, t in moves]
        pairs = [(s * cols + (owner + step) % cols, t * cols + owner) for s, t, owner in owners]
        arrived.append(lax.ppermute(values, (ROW, COL), pairs))
    first = lax.axis_index(COL) == 0
    return jnp.stack([jnp.where(first, arrived[0], arrived[1]), jnp.where(first, arrived[1], arrived[0])])


def ladder_by_plane_sums(amplitudes, integrals):
    plane = lax.axis_index(ROW)
    end = lax.axis_size(ROW) - 1
    early, late = streamed_blocks(amplitudes, integrals)
    held = to_owner_col(plane_sums(early))
    above = between_planes(held[:, 1], [(p, p + 1) for p in range(end)])
    below = between_planes(held[:, 2], [(p + 1, p) for p in range(end)])
    inner = (plane > 0) & (plane < end)
    last, lent_last, second, lent_near = plane_sums(late)
    lent_self = to_owner_col(second)
    three = to_owner(jnp.where(inner, lent_near, last), [(0, end), (1, 2), (2, 1), (end, 0)])
    two = jnp.where(inner, jnp.stack([last, lent_last]), jnp.stack([second, jnp.zeros_like(second)]))
    two = to_owner(two, [(0, 2), (1, end), (2, 0), (end, 1)])
    even = held[:, 0] + two[:, 0] + jnp.where(inner, three, 0.0)
    odd = above + below + two[:, 1] + jnp.where(inner, lent_self, three)
    own_first = plane % 2 == 0
    owned = jnp.stack([jnp.where(own_first, even, odd), jnp.where(own_first, odd, even)])
    group, cols, share, height = owned.shape
    return owned.transpose(0, 3, 1, 2).reshape(group * height, cols * share)


def ladder_by_scatter(amplitudes, integrals):
    partial_rows = jnp.dot(
        amplitudes,
        lax.all_gather(integrals, ROW, axis=1, tiled=True),
        precision=lax.Precision.HIGHEST,
        preferred_element_type=jnp.float32,
    )
    partial_sum = lax.all_to_all(partial_rows, ROW, split_axis=1, concat_axis=0, tiled=True)
    col_count = lax.axis_size(COL)
    layer_count = lax.axis_size(LAYER)
    pair_rows = partial_sum.shape[0] // col_count
    slab_cols = partial_sum.shape[1] // layer_count
    blocks = partial_sum.reshape(col_count, pair_rows, layer_count, slab_cols)
    blocks = blocks.transpose(0, 2, 1, 3).reshape(col_count * layer_count * pair_rows, slab_cols)
    return lax.psum_scatter(blocks, (COL, LAYER), scatter_dimension=0, tiled=True)


def denominators(occ_energy, vir_energy, pair_rows, slab_cols):
    occupied = occ_energy.shape[0]
    virtuals = vir_energy.shape[0]
    first_np, second_np = np.triu_indices(occupied, 1)
    ij_start = lax.axis_index(COL) * pair_rows
    ab_start = (
        lax.axis_index(ROW) * lax.axis_size(LAYER) + lax.axis_index(LAYER)
    ) * slab_cols
    first_index = lax.dynamic_slice_in_dim(
        jnp.asarray(first_np, dtype=jnp.int32), ij_start, pair_rows
    )
    second_index = lax.dynamic_slice_in_dim(
        jnp.asarray(second_np, dtype=jnp.int32), ij_start, pair_rows
    )
    pair_sum = lookup(first_index, occ_energy) + lookup(second_index, occ_energy)
    ab_index = ab_start + jnp.arange(slab_cols, dtype=jnp.int32)
    vir_sum = lookup(ab_index // virtuals, vir_energy) + lookup(ab_index % virtuals, vir_energy)
    return pair_sum[:, None] - vir_sum[None, :]


def sums_fit(size_of):
    return size_of(ROW) == 4 and size_of(COL) == 2 and size_of(LAYER) % 2 == 0


def shards(amplitudes, integrals, occ_energy, vir_energy):
    if sums_fit(lax.axis_size):
        ladder = ladder_by_plane_sums(amplitudes, integrals)
    else:
        ladder = ladder_by_scatter(amplitudes, integrals)
    denominator = denominators(occ_energy, vir_energy, ladder.shape[0], ladder.shape[1])
    return (ladder, ladder / denominator)


def solution(mesh):
    in_specs = (P(ROW, (LAYER, COL)), P((LAYER, COL), ROW), P(), P())
    out_specs = (P(COL, (ROW, LAYER)), P(COL, (ROW, LAYER)))
    step = jax.shard_map(shards, mesh=mesh, in_specs=in_specs, out_specs=out_specs, check_vma=False)
    if not sums_fit(mesh.shape.__getitem__):
        return step
    return step
```

```python
import functools

import jax
import jax.numpy as jnp
import numpy as np
from jax import lax
from jax.experimental import pallas as pl
from jax.experimental.pallas import tpu as pltpu
from jax.sharding import PartitionSpec as P


ROW, COL, LAYER = "row", "col", "layer"


def lookup(indices, values_table):
    positions = jnp.arange(values_table.shape[0], dtype=jnp.int32)
    picked = jnp.where(indices[:, None] == positions[None, :], values_table[None, :], 0.0)
    return jnp.sum(picked, axis=1)


def split(values):
    high = values.astype(jnp.bfloat16)
    return high, (values - high.astype(jnp.float32)).astype(jnp.bfloat16)


def product_kernel(depth, step, term_sizes, flag_ref, *refs):
    at = pl.program_id(0)
    term_refs = refs[: sum(term_sizes)]
    source_ref = refs[len(term_refs)]
    start_refs = refs[len(term_refs) + 1 : -1]
    total_ref = refs[-1]

    def valid(values):
        if depth % step == 0:
            return values
        place = lax.broadcasted_iota(jnp.int32, values.shape, 1)
        return jnp.where(place < depth - at * step, values, 0.0)

    blocks = []
    used = 0
    for size in term_sizes:
        block = term_refs[used][...]
        if size == 2:
            other = term_refs[used + 1][...]
            block = jnp.where(flag_ref[0] == 2, block + other, jnp.where(flag_ref[0] == 1, other, block))
        blocks.append(split(valid(block)))
        used += size
    high, low = split(valid(source_ref[...]))

    def dot(a, b):
        return lax.dot_general(a, b, (((1,), (1,)), ((), ())), preferred_element_type=jnp.float32)

    left_high = jnp.concatenate([block for block, _ in blocks], axis=0)
    left = jnp.concatenate([left_high] + [block for _, block in blocks], axis=0)
    half = left_high.shape[0]
    both = dot(left, high)
    part = both[:half] + (both[half:] + dot(left_high, low))

    @pl.when(at == 0)
    def _():
        total_ref[...] = part if not start_refs else start_refs[0][...] + part

    @pl.when(at > 0)
    def _():
        total_ref[...] += part


def products(terms, source, offset, start=None, flag=None):
    chunks = [chunk for term in terms for chunk in term]
    depth, columns = chunks[0].shape
    height = source.shape[0]
    step = next(n for n in (512, 256, 128) if offset % n == 0)
    if depth % step and depth % 256 == 0:
        step = 256
    in_specs = [pl.BlockSpec((columns, step), lambda i, _: (0, i))] * len(chunks)
    in_specs.append(pl.BlockSpec((height, step), lambda i, _: (0, offset // step + i)))
    shape = (len(terms) * columns, height)
    whole = pl.BlockSpec(shape, lambda i, _: (0, 0))
    operands = [chunk.T for chunk in chunks] + [source]
    aliases = {}
    if start is not None:
        aliases = {1 + len(operands): 0}
        in_specs.append(whole)
        operands.append(start)
    flags = jnp.full((1,), 2, jnp.int32) if flag is None else flag.reshape(1).astype(jnp.int32)
    return pl.pallas_call(
        functools.partial(product_kernel, depth, step, tuple(len(t) for t in terms)),
        grid_spec=pltpu.PrefetchScalarGridSpec(
            num_scalar_prefetch=1,
            grid=(pl.cdiv(depth, step),),
            in_specs=in_specs,
            out_specs=whole,
        ),
        out_shape=jax.ShapeDtypeStruct(shape, jnp.float32),
        input_output_aliases=aliases,
        compiler_params=pltpu.CompilerParams(dimension_semantics=("arbitrary",)),
        cost_estimate=pl.CostEstimate(
            flops=2 * depth * shape[0] * height,
            bytes_accessed=4 * depth * (columns * len(chunks) + height),
            transcendentals=0,
        ),
    )(flags, *operands)


def product(chunk, source):
    return lax.dot_general(
        chunk,
        source,
        (((0,), (1,)), ((), ())),
        precision=lax.Precision.HIGH,
        preferred_element_type=jnp.float32,
    )


def total(parts):
    return sum(parts[1:], parts[0])


CHUNKS = 5
KEPT = 2
LOANS = ((2, 3), (4,))


def chunk_bounds(depth):
    tile = 256
    ends = [depth * share // 1024 // tile * tile for share in (314, 656, 799, 913)]
    return [0] + ends + [depth]


def streamed_blocks(amplitudes, integrals):
    rows = lax.axis_size(ROW)
    plane = lax.axis_index(ROW)
    bounds = chunk_bounds(integrals.shape[0])
    own = [integrals[a:b] for a, b in zip(bounds[:-1], bounds[1:])]

    def hop(values, distance, c):
        low, high = (0, rows - 1) if c < KEPT else (1, rows - 2)
        up = [(p - 1, p) for p in range(distance, rows) if low <= p <= high]
        down = [(rows - 1 - p, rows - 1 - t) for p, t in up]
        upward = lax.ppermute(values[0], ROW, up)
        downward = lax.ppermute(values[1], ROW, down)
        return upward, downward

    near, lent = [], {}
    for c in range(CHUNKS):
        near.append(hop((own[c], own[c]), 1, c))
    for group in LOANS:
        first = bounds[group[0]]
        sent = amplitudes[:, first : bounds[group[-1] + 1]]
        loan = lax.ppermute(sent, ROW, [(0, 1), (rows - 1, rows - 2)])
        for c in group:
            lent[c] = (loan, bounds[c] - first)

    def lent_part(c):
        loan, offset = lent[c]
        return loan[:, offset : offset + bounds[c + 1] - bounds[c]]

    middle = [hop(near[c], 2, c) for c in range(CHUNKS)]
    joined = [lax.optimization_barrier(total(middle[c])) for c in range(KEPT)]
    far = []
    for c in range(KEPT):
        far.append(lax.ppermute(joined[c], ROW, [(1, 0), (rows - 2, rows - 1)]))

    lower = (plane < rows // 2).astype(jnp.int32)
    at_end = (plane == 0) | (plane == rows - 1)
    slab = integrals.shape[1]
    self_block = products([(integrals,)], amplitudes, 0)
    nearby, second, lent_inner = None, None, None
    for c in range(CHUNKS):
        nearby = products([(near[c][0],), (near[c][1],)], amplitudes, bounds[c], nearby)
    for c in range(KEPT - 1):
        second = products([(joined[c],)], amplitudes, bounds[c], second)
    a, b = bounds[KEPT - 1 : KEPT + 1]
    second = second + product(joined[KEPT - 1], amplitudes[:, a:b])
    second = lax.optimization_barrier(second)
    end = CHUNKS - 1
    for c in range(KEPT, end):
        lent_inner = products([(own[c],), near[c]], *lent[c], lent_inner, lower)
    late = jnp.where(at_end, 0.0, second)
    second = jnp.where(at_end, second, 0.0)
    for c in range(KEPT - 1):
        late = late + product(far[c], amplitudes[:, bounds[c] : bounds[c + 1]])
    late = lax.optimization_barrier(late)
    lent_late = 0.0
    for c in range(KEPT, end):
        chunk = total(middle[c])
        late = late + product(chunk, amplitudes[:, bounds[c] : bounds[c + 1]])
        lent_late = lent_late + product(chunk, lent_part(c))
        late, lent_late = lax.optimization_barrier((late, lent_late))
    chosen = jnp.where(plane < rows // 2, near[end][1], near[end][0])
    lent_self = lent_inner[:slab] + product(own[end], lent_part(end))
    lent_near = lent_inner[slab:] + product(chosen, lent_part(end))
    late = late + product(far[KEPT - 1], amplitudes[:, a:b])
    chunk = total(middle[end])
    late = late + product(chunk, amplitudes[:, bounds[end] :])
    lent_late = lent_late + product(chunk, lent_part(end))
    return (self_block, nearby[slab:], nearby[:slab]), (late, lent_late, second + lent_self, lent_near)


def plane_sums(blocks):
    layers, cols = lax.axis_size(LAYER), lax.axis_size(COL)
    layer, col = lax.axis_index(LAYER), lax.axis_index(COL)
    share = blocks[0].shape[0] // (layers * cols)
    pairs = layers // 2
    stacked = jnp.stack(blocks).reshape(len(blocks), pairs, 2, cols, share, -1)

    def pick(values, place, axis):
        return lax.dynamic_index_in_dim(values, place, axis, keepdims=False)

    core = layer % 2
    other = lax.ppermute(pick(stacked, 1 - core, 2), LAYER, [(n, n ^ 1) for n in range(layers)])
    halves = pick(stacked, core, 2) + other
    pair = layer // 2

    def piece(pair_at, col_at):
        return pick(pick(halves, pair_at, 1), col_at, 1)

    sums = piece(pair, col)
    for pair_step in range(pairs):
        for col_step in range(cols):
            if pair_step or col_step:
                moves = [
                    (
                        c * layers + n,
                        (c + col_step) % cols * layers + ((n // 2 + pair_step) % pairs) * 2 + n % 2,
                    )
                    for c in range(cols)
                    for n in range(layers)
                ]
                sent = piece((pair + pair_step) % pairs, (col + col_step) % cols)
                sums = sums + lax.ppermute(sent, (COL, LAYER), moves)
    return sums


def to_owner_col(values):
    rows, cols = lax.axis_size(ROW), lax.axis_size(COL)
    col, plane = lax.axis_index(COL), lax.axis_index(ROW)
    owners = [p * cols // rows for p in range(rows)]
    pairs = [(p * cols + (owners[p] + 1) % cols, p * cols + owners[p]) for p in range(rows)]
    other = lax.ppermute(values, (ROW, COL), pairs)
    first = col == 0
    both = jnp.stack([jnp.where(first, values, other), jnp.where(first, other, values)])
    return jnp.where(col == plane * cols // rows, both, 0.0)


def between_planes(values, moves):
    rows, cols = lax.axis_size(ROW), lax.axis_size(COL)
    pairs = [(s * cols + s * cols // rows, t * cols + s * cols // rows) for s, t in moves]
    return lax.ppermute(values, (ROW, COL), pairs)


def to_owner(values, moves):
    rows, cols = lax.axis_size(ROW), lax.axis_size(COL)
    arrived = []
    for step in range(cols):
        owners = [(s, t, s * cols // rows) for s, t in moves]
        pairs = [(s * cols + (owner + step) % cols, t * cols + owner) for s, t, owner in owners]
        arrived.append(lax.ppermute(values, (ROW, COL), pairs))
    first = lax.axis_index(COL) == 0
    return jnp.stack([jnp.where(first, arrived[0], arrived[1]), jnp.where(first, arrived[1], arrived[0])])


def ladder_by_plane_sums(amplitudes, integrals):
    plane = lax.axis_index(ROW)
    end = lax.axis_size(ROW) - 1
    early, late = streamed_blocks(amplitudes, integrals)
    held = to_owner_col(plane_sums(early))
    above = between_planes(held[:, 1], [(p, p + 1) for p in range(end)])
    below = between_planes(held[:, 2], [(p + 1, p) for p in range(end)])
    inner = (plane > 0) & (plane < end)
    last, lent_last, second, lent_near = plane_sums(late)
    lent_self = to_owner_col(second)
    three = to_owner(jnp.where(inner, lent_near, last), [(0, end), (1, 2), (2, 1), (end, 0)])
    two = jnp.where(inner, jnp.stack([last, lent_last]), jnp.stack([second, jnp.zeros_like(second)]))
    two = to_owner(two, [(0, 2), (1, end), (2, 0), (end, 1)])
    even = held[:, 0] + two[:, 0] + jnp.where(inner, three, 0.0)
    odd = above + below + two[:, 1] + jnp.where(inner, lent_self, three)
    own_first = plane % 2 == 0
    owned = jnp.stack([jnp.where(own_first, even, odd), jnp.where(own_first, odd, even)])
    group, cols, share, height = owned.shape
    return owned.transpose(0, 3, 1, 2).reshape(group * height, cols * share)


def ladder_by_scatter(amplitudes, integrals):
    partial_rows = jnp.dot(
        amplitudes,
        lax.all_gather(integrals, ROW, axis=1, tiled=True),
        precision=lax.Precision.HIGHEST,
        preferred_element_type=jnp.float32,
    )
    partial_sum = lax.all_to_all(partial_rows, ROW, split_axis=1, concat_axis=0, tiled=True)
    col_count = lax.axis_size(COL)
    layer_count = lax.axis_size(LAYER)
    pair_rows = partial_sum.shape[0] // col_count
    slab_cols = partial_sum.shape[1] // layer_count
    blocks = partial_sum.reshape(col_count, pair_rows, layer_count, slab_cols)
    blocks = blocks.transpose(0, 2, 1, 3).reshape(col_count * layer_count * pair_rows, slab_cols)
    return lax.psum_scatter(blocks, (COL, LAYER), scatter_dimension=0, tiled=True)


def denominators(occ_energy, vir_energy, pair_rows, slab_cols):
    occupied = occ_energy.shape[0]
    virtuals = vir_energy.shape[0]
    first_np, second_np = np.triu_indices(occupied, 1)
    ij_start = lax.axis_index(COL) * pair_rows
    ab_start = (
        lax.axis_index(ROW) * lax.axis_size(LAYER) + lax.axis_index(LAYER)
    ) * slab_cols
    first_index = lax.dynamic_slice_in_dim(
        jnp.asarray(first_np, dtype=jnp.int32), ij_start, pair_rows
    )
    second_index = lax.dynamic_slice_in_dim(
        jnp.asarray(second_np, dtype=jnp.int32), ij_start, pair_rows
    )
    pair_sum = lookup(first_index, occ_energy) + lookup(second_index, occ_energy)
    ab_index = ab_start + jnp.arange(slab_cols, dtype=jnp.int32)
    vir_sum = lookup(ab_index // virtuals, vir_energy) + lookup(ab_index % virtuals, vir_energy)
    return pair_sum[:, None] - vir_sum[None, :]


def sums_fit(size_of):
    return size_of(ROW) == 4 and size_of(COL) == 2 and size_of(LAYER) % 2 == 0


def shards(amplitudes, integrals, occ_energy, vir_energy):
    if sums_fit(lax.axis_size):
        ladder = ladder_by_plane_sums(amplitudes, integrals)
    else:
        ladder = ladder_by_scatter(amplitudes, integrals)
    denominator = denominators(occ_energy, vir_energy, ladder.shape[0], ladder.shape[1])
    return (ladder, ladder / denominator)


def solution(mesh):
    in_specs = (P(ROW, (LAYER, COL)), P((LAYER, COL), ROW), P(), P())
    out_specs = (P(COL, (ROW, LAYER)), P(COL, (ROW, LAYER)))
    step = jax.shard_map(shards, mesh=mesh, in_specs=in_specs, out_specs=out_specs, check_vma=False)
    if not sums_fit(mesh.shape.__getitem__):
        return step
    return step
```
